1024 devices in a mesh: grp: 64 (over y, x_lo, core), tile: 16 (over z, x_hi).
Axes of the slice: x: 8 (x_hi: 2, x_lo: 4; x = x_hi * 4 + x_lo), y: 8, z: 8, core: 2. Of those that a mesh axis runs over, the one named last changes fastest.
Arguments:
- atm_flux: float32 [6, 1048576], P(None, ('grp', 'tile')), may hold values from -6 to 6
- send_block: int32 [1024, 16, 4], P(('grp', 'tile')), may hold values from 0 to 7
- send_count: int32 [1024, 16], P(('grp', 'tile')), may hold values from 1 to 4, as said below
- recv_block: int32 [1024, 16, 4], P(('grp', 'tile')), may hold values from 0 to 63
- recv_weight: bfloat16 [1024, 16, 4, 128, 128], P(('grp', 'tile')), may hold values from -0.5 to 0.5
- sea_temp: float32 [2048, 4096], P('grp', 'tile'), may hold values from -6 to 6
- ocean_mask: int32 [2048, 4096], P('grp', 'tile'), may hold values 0 or 1
Outputs:
- heat_flux: float32 [2048, 4096], P('grp', 'tile')
- stress_curl: float32 [2048, 4096], P('grp', 'tile')
- atm_return: float32 [4, 1048576], P(None, ('grp', 'tile'))
The draws below stay inside these ranges and needn't reach their ends.
Inputs may be any that keep to these rules, and one draw needn't show every extreme that they name: `send_count`: in every draw a quarter of the tile indices, drawn from the seed, receive exactly 4 blocks from every device of their group; every other pair carries 1 to 2 blocks.
All inputs are finite; a program needn't handle non-finite values. No bound on the sum of `ocean_mask` on one device may be relied on, other than what follows from the above.
Results may differ from the reference program's by a relative error of at most 0.0003.
Values sent between devices are 32-bit elements; how exact they have to be, the bound alone decides.
A program may use at most 32 MiB of HBM per device.

```python
import jax
import jax.numpy as jnp
from jax import lax

NF = 6
NB = 4
BLK = 128
CAP = 4
ABLK_DEV = 8
OROW = 32
OCOL = 256
OBLK = 64
NYO = 2048
NXO = 4096
ACELLS = 1048576
N_GRP = 64
N_TILE = 16
DEVICES = 1024


def draw_send_count(key, part):
    first_key, second_key = jax.random.split(jax.random.fold_in(key, 11))
    base_count = jax.random.randint(first_key, (DEVICES, N_TILE), 1, CAP // 2 + 1)
    offset = jax.random.randint(second_key, (), 0, 4)
    column = jnp.arange(N_TILE, dtype=jnp.int32)
    busy = ((column + offset) % 4 == 0)[None, :]
    return jnp.where(busy, CAP, base_count).astype(jnp.int32)


def set_ends(drawn, key, least, high):
    longest = drawn.shape.index(max(drawn.shape))
    spots = []
    for shift in (0, 1):
        where = [jax.random.randint(jax.random.fold_in(key, axis), (), 0, length) for axis, length in enumerate(drawn.shape)]
        where[longest] = (where[longest] + shift) % drawn.shape[longest]
        spots.append(tuple(where))
    return drawn.at[spots[0]].set(least).at[spots[1]].set(high)


def shard_levels(stream_key, extent, cuts, smallest, largest):
    def one(dim, parts):
        heights = jax.random.uniform(jax.random.fold_in(jax.random.fold_in(stream_key, 6), dim), (parts,), jnp.float32, smallest / len(cuts), largest / len(cuts))
        return jnp.repeat(jnp.exp(heights), extent[dim] // parts).reshape((-1,) + (1,) * (len(extent) - dim - 1))

    loudness = one(*cuts[0])
    for cut in cuts[1:]:
        loudness = loudness * one(*cut)
    return loudness


def noise(key, extent, deviation, reach, cuts=(), kind=jnp.bfloat16):
    values = deviation * jax.random.normal(key, extent, jnp.float32)
    if cuts:
        values = values * shard_levels(key, extent, cuts, -0.22, 0.18)
    return jnp.clip(values, -reach, reach).astype(kind)


def setup_inputs(seed: int = 0) -> dict:
    key_of = jax.random.split(jax.random.key(seed), 8)
    return {
        "atm_flux": noise(key_of[0], (NF, ACELLS), 1.0, 6.0, ((1, 1024),), jnp.float32),
        "send_block": set_ends(jax.random.randint(key_of[1], (DEVICES, N_TILE, CAP), 0, ABLK_DEV), jax.random.fold_in(key_of[1], 1), 0, ABLK_DEV - 1).astype(jnp.int32),
        "send_count": draw_send_count(jax.random.fold_in(key_of[7], 71), 0),
        "recv_block": set_ends(jax.random.randint(key_of[3], (DEVICES, N_TILE, CAP), 0, OBLK), jax.random.fold_in(key_of[3], 1), 0, OBLK - 1).astype(jnp.int32),
        "recv_weight": noise(key_of[4], (DEVICES, N_TILE, CAP, BLK, BLK), BLK ** -0.5, 0.5, ((0, 1024),)),
        "sea_temp": noise(key_of[5], (NYO, NXO), 1.0, 6.0, ((0, 64), (1, 16)), jnp.float32),
        "ocean_mask": set_ends((jax.random.randint(key_of[6], (NYO, NXO), 0, 10) < 7).astype(jnp.int32), jax.random.fold_in(key_of[6], 1), 0, 1),
    }


precise = lax.Precision.HIGHEST

def bulk_formula(fields, surface_temp, ocean_mask):
    sea_share = ocean_mask.astype(jnp.float32)
    wind_u, wind_v, air_temp, air_vapor, short_down, long_down = [fields[k] for k in range(6)]
    wind_speed = jnp.sqrt(wind_u * wind_u + wind_v * wind_v + 0.5)
    stress_x = 0.8 * wind_speed * wind_u * sea_share
    stress_y = 0.8 * wind_speed * wind_v * sea_share
    sensible = 0.6 * wind_speed * (surface_temp - air_temp)
    latent = 0.7 * wind_speed * (jnp.exp(0.3 * surface_temp) - air_vapor)
    long_up = 0.4 * (1.0 + 0.2 * surface_temp) ** 4
    heat_flux = (0.94 * short_down + long_down - long_up - sensible - latent) * sea_share
    surface = jnp.stack([surface_temp, sensible, latent, long_up]) * sea_share[None]
    return (stress_x, stress_y, heat_flux, surface)

def reference(atm_flux, send_block, send_count, recv_block, recv_weight, sea_temp, ocean_mask):
    group_count = N_GRP
    tile_count = N_TILE
    device_count = group_count * tile_count
    slot_range = jnp.arange(CAP, dtype=jnp.int32)
    blocks = atm_flux.reshape(NF, device_count, ABLK_DEV, BLK)

    def pick_slots(dev_blocks, send_index, pair_count):
        chosen = jnp.take(dev_blocks, send_index, axis=1)
        live_slots = (slot_range[None, :] < pair_count[:, None]).astype(jnp.float32)
        return chosen * live_slots[None, :, :, None]
    picked = jax.vmap(pick_slots, in_axes=(1, 0, 0))(blocks, send_block, send_count)
    picked = picked.reshape(group_count, tile_count, NF, tile_count, CAP, BLK)
    arrived = jnp.transpose(picked, (0, 3, 1, 4, 2, 5)).reshape(device_count, tile_count, CAP, NF, BLK)

    def remap_in(entries):
        weight, dest_block, incoming = entries
        weight_wide = weight.astype(jnp.float32)
        remapped = jnp.einsum('scij,scfj->scfi', weight_wide, incoming, precision=precise)
        onehot = (jnp.arange(OBLK, dtype=jnp.int32)[:, None] == dest_block.reshape(-1)[None, :]).astype(jnp.float32)
        landed = jnp.dot(onehot, remapped.reshape(tile_count * CAP, NF * BLK), precision=precise)
        return landed.reshape(OBLK, NF, BLK)
    landed = lax.map(remap_in, (recv_weight, recv_block, arrived))
    grid = landed.reshape(group_count, tile_count, OBLK, NF, BLK).transpose(3, 0, 1, 2, 4)
    grid = grid.reshape(NF, group_count, tile_count, OROW, OCOL).transpose(0, 1, 3, 2, 4).reshape(NF, NYO, NXO)
    stress_x, stress_y, heat_flux, surface = bulk_formula(grid, sea_temp, ocean_mask)
    sea_share = ocean_mask.astype(jnp.float32)
    fold_values = -jnp.flip(stress_x[NYO - 1])
    column_x = jnp.concatenate([jnp.zeros((1, NXO), jnp.float32), stress_x, fold_values[None]], axis=0)
    stress_curl = 0.5 * (jnp.roll(stress_y, -1, axis=1) - jnp.roll(stress_y, 1, axis=1)) - 0.5 * (column_x[2:] - column_x[:-2])
    stress_curl = stress_curl * sea_share
    per_device = surface.reshape(NB, group_count, OROW, tile_count, OCOL).transpose(1, 3, 0, 2, 4)
    per_device = per_device.reshape(device_count, NB, OBLK, BLK)

    def remap_out(entries):
        weight, dest_block, ocean_blocks = entries
        weight_wide = weight.astype(jnp.float32)
        chosen = jnp.take(ocean_blocks, dest_block, axis=1)
        return jnp.einsum('scij,fsci->scfj', weight_wide, chosen, precision=precise)
    returned = lax.map(remap_out, (recv_weight, recv_block, per_device))
    returned = returned.reshape(group_count, tile_count, tile_count, CAP, NB, BLK).transpose(0, 2, 1, 3, 4, 5)
    returned = returned.reshape(device_count, tile_count, CAP, NB, BLK)

    def gather_back(send_index, pair_count, pieces):
        live_slots = (slot_range[None, :] < pair_count[:, None]).astype(jnp.float32)
        pieces = pieces * live_slots[:, :, None, None]
        onehot = (jnp.arange(ABLK_DEV, dtype=jnp.int32)[:, None] == send_index.reshape(-1)[None, :]).astype(jnp.float32)
        total = jnp.dot(onehot, pieces.reshape(tile_count * CAP, NB * BLK), precision=precise)
        return total.reshape(ABLK_DEV, NB, BLK)
    atm_parts = jax.vmap(gather_back)(send_block, send_count, returned)
    atm_return = atm_parts.transpose(2, 0, 1, 3).reshape(NB, ACELLS)
    return (heat_flux, stress_curl, atm_return)
```

```python
import functools

import jax
import jax.numpy as jnp
from jax import lax
from jax.experimental import pallas as pl
from jax.experimental.pallas import tpu as pltpu
from jax.sharding import PartitionSpec as P

MESH = pl.DeviceIdType.MESH
F32 = jnp.float32
BF16 = jnp.bfloat16
NZ = 8
N_TILE = 16
N_GRP = 64
CAP = 4
NF = 6
NB = 4
LANES = 128
OFFSETS = sorted(
    [(dz, dx) for dz in range(NZ) for dx in range(2)],
    key=lambda o: (min(o[0], NZ - o[0]) + 4 * o[1], o),
)
FAR_FIRST = list(range(N_TILE - 1, 0, -1))


def split(value):
    high = value.astype(BF16).astype(F32)
    return high, value - high


def exchange(
    atm_hbm, sb_ref, sc_ref, rb_ref, w_hbm, temp_hbm, mask_hbm,
    heat_ref, curl_ref, back_ref,
    atm, tiles, w, temp, mask, send, recv, rows, surf, ret_send, ret_recv, sxp, halo_send, halo_recv,
    in_sem, fs_sem, fr_sem, bs_sem, br_sem, hs_sem, hr_sem,
):
    g = lax.axis_index("grp")
    t = lax.axis_index("tile")
    z, half = t // 2, lax.rem(t, 2)

    def to_peer(k):
        dz, dx = OFFSETS[k]
        return lax.rem(z + dz, NZ) * 2 + (1 - half if dx else half)

    def from_peer(k):
        dz, dx = OFFSETS[k]
        return lax.rem(z + NZ - dz, NZ) * 2 + (1 - half if dx else half)

    loads = [
        pltpu.make_async_copy(atm_hbm, atm, in_sem.at[0]),
        pltpu.make_async_copy(w_hbm, w, in_sem.at[1]),
        pltpu.make_async_copy(temp_hbm, temp, in_sem.at[2]),
        pltpu.make_async_copy(mask_hbm, mask, in_sem.at[3]),
    ]
    barrier = pltpu.get_barrier_semaphore()
    north, south = lax.rem(g + 1, N_GRP), lax.rem(g + N_GRP - 1, N_GRP)
    for k in FAR_FIRST:
        pl.semaphore_signal(barrier, 1, device_id=(g, to_peer(k)), device_id_type=MESH)
    for other in (north, south):
        pl.semaphore_signal(barrier, 1, device_id=(other, t), device_id_type=MESH)
    for load in loads:
        load.start()

    lane = lax.broadcasted_iota(jnp.int32, (8, LANES), 1)
    dest = jnp.full((8, LANES), -1, jnp.int32)
    for k in range(N_TILE):
        s = from_peer(k)
        for c in range(CAP):
            slot = k * CAP + c
            dest = jnp.where(lax.rem(lane, 64) == slot, rb_ref[c, s], dest)
    row64 = lax.broadcasted_iota(jnp.int32, (64, LANES), 0)
    block_of_row = 2 * lax.rem(row64, 32) + row64 // 32
    dest64 = jnp.concatenate([dest] * 8, axis=0)
    land = jnp.where(block_of_row == dest64, 1.0, 0.0).astype(BF16)
    picks = []
    for part in range(2):
        pick = jnp.full((8, LANES), -1, jnp.int32)
        for k in range(8 * part, 8 * part + 8):
            u = to_peer(k)
            count = jnp.full((8, LANES), sc_ref[0, u], jnp.int32)
            for c in range(CAP):
                mine = (lane // NB == (k - 8 * part) * CAP + c) & (count > c)
                pick = jnp.where(mine, sb_ref[c, u], pick)
        row32 = lax.broadcasted_iota(jnp.int32, (32, LANES), 0)
        lane32 = lax.broadcasted_iota(jnp.int32, (32, LANES), 1)
        pick32 = jnp.concatenate([pick] * 4, axis=0)
        hit = (row32 // NB == pick32) & (lax.rem(row32, NB) == lax.rem(lane32, NB))
        picks.append(jnp.where(hit, 1.0, 0.0).astype(BF16))
    gather_back = jnp.concatenate(picks, axis=1)

    surf[...] = jnp.zeros_like(surf)
    loads[0].wait()
    for b in range(8):
        tiles[b] = atm[:, b * LANES:(b + 1) * LANES]
    for k in range(N_TILE):
        u = to_peer(k)
        count = jnp.full((NF, LANES), sc_ref[0, u], jnp.int32)
        for c in range(CAP):
            send[k, c * NF:(c + 1) * NF, :] = jnp.where(count > c, tiles[sb_ref[c, u]], 0.0)

    pl.semaphore_wait(barrier, N_TILE + 1)
    forward = {}
    for k in FAR_FIRST:
        forward[k] = pltpu.make_async_remote_copy(
            src_ref=send.at[k], dst_ref=recv.at[k], send_sem=fs_sem.at[k], recv_sem=fr_sem.at[k],
            device_id=(g, to_peer(k)), device_id_type=MESH,
        )
        forward[k].start()
    for load in loads[1:]:
        load.wait()

    zeros2 = jnp.zeros((2, LANES), F32)
    for k in range(N_TILE):
        s = from_peer(k)
        if k:
            forward[k].wait_recv()
        source = recv if k else send
        for c in range(CAP):
            value = source[k, c * NF:(c + 1) * NF, :]
            high, low = split(value)
            lhs = jnp.concatenate([high, zeros2, low, zeros2], axis=0).astype(BF16)
            out = lax.dot_general(lhs, w[s, c], (((1,), (1,)), ((), ())), preferred_element_type=F32)
            at = (k * CAP + c) * 8
            rows[at:at + 8, :] = out[:8] + out[8:]

    def landed(f):
        high, low = split(rows[pl.ds(f, 64, stride=8), :])
        rhs = jnp.concatenate([high, low], axis=0).astype(BF16)
        return jnp.dot(land, rhs, preferred_element_type=F32)

    wind_u, wind_v, air_temp, air_vapor, short_down, long_down = [landed(f) for f in range(NF)]
    sea = jnp.concatenate([temp[:, :LANES], temp[:, LANES:]], axis=0)
    share = jnp.concatenate([mask[:, :LANES], mask[:, LANES:]], axis=0).astype(F32)
    speed = jnp.sqrt(wind_u * wind_u + wind_v * wind_v + 0.5)
    sensible = 0.6 * speed * (sea - air_temp)
    latent = 0.7 * speed * (jnp.exp(0.3 * sea) - air_vapor)
    base = 1.0 + 0.2 * sea
    long_up = 0.4 * ((base * base) * (base * base))
    for f, value in enumerate((sea, sensible, latent, long_up)):
        value = value * share
        for h in range(2):
            surf[pl.ds(h, 32, stride=2), f, :] = value[32 * h:32 * h + 32]

    stress_x = 0.8 * speed * wind_u * share
    stress_y = 0.8 * speed * wind_v * share
    heat_ref[...] = (0.94 * short_down + long_down - long_up - sensible - latent) * share

    back = {}

    def start_back(k):
        if k:
            back[k] = pltpu.make_async_remote_copy(
                src_ref=ret_send.at[k], dst_ref=ret_recv.at[k], send_sem=bs_sem.at[k], recv_sem=br_sem.at[k],
                device_id=(g, from_peer(k)), device_id_type=MESH,
            )
            back[k].start()

    order = FAR_FIRST + [0]
    for i, k in enumerate(order):
        s = from_peer(k)
        for c in range(CAP):
            high, low = split(surf[rb_ref[c, s]])
            lhs = jnp.concatenate([high, low], axis=0).astype(BF16)
            out = jnp.dot(lhs, w[s, c], preferred_element_type=F32)
            total = out[:8] + out[8:]
            if k:
                ret_send[k, c * NB:(c + 1) * NB, :] = total[:NB]
            else:
                ret_recv[0, c * NB:(c + 1) * NB, :] = total[:NB]
        if i:
            start_back(order[i - 1])

    left_y, right_y = stress_y[:32], stress_y[32:]
    to_east = jnp.zeros((8, LANES), F32)
    to_west = jnp.zeros((8, LANES), F32)
    for a in range(4):
        east = pltpu.roll(right_y[8 * a:8 * a + 8], a + 1, 1)
        west = left_y[8 * a:8 * a + 8]
        if a:
            west = pltpu.roll(west, a, 1)
        to_east = jnp.where(lane == a, east, to_east)
        to_west = jnp.where(lane == a, west, to_west)
    sxp[0, 8:40, :] = stress_x[:32]
    sxp[1, 8:40, :] = stress_x[32:]
    zeros6 = jnp.zeros((6, LANES), F32)
    top = jnp.concatenate([stress_x[31:32], stress_x[63:64], zeros6], axis=0)
    bottom = jnp.concatenate([stress_x[0:1], stress_x[32:33], zeros6], axis=0)
    halo_send[0] = top
    halo_send[1] = bottom
    halo_send[2] = to_east
    halo_send[3] = to_west
    start_back(0)
    t_next, t_last = lax.rem(t + 1, N_TILE), lax.rem(t + N_TILE - 1, N_TILE)
    targets = ((0, north, t), (1, south, t), (2, g, t_next), (3, g, t_last), (0, g, N_TILE - 1 - t))
    halos = []
    for i, (source, gg, tt) in enumerate(targets):
        copy = pltpu.make_async_remote_copy(
            src_ref=halo_send.at[source], dst_ref=halo_recv.at[i], send_sem=hs_sem.at[i], recv_sem=hr_sem.at[i],
            device_id=(gg, tt), device_id_type=MESH,
        )
        copy.start()
        halos.append(copy)
    for copy in halos:
        copy.wait_recv()

    fold = halo_recv[4]
    first = fold.astype(BF16)
    second = (fold - first.astype(F32)).astype(BF16)
    third = (fold - first.astype(F32) - second.astype(F32)).astype(BF16)
    ri = lax.broadcasted_iota(jnp.int32, (LANES, LANES), 0)
    ci = lax.broadcasted_iota(jnp.int32, (LANES, LANES), 1)
    mirror = jnp.where(ri + ci == LANES - 1, 1.0, 0.0).astype(BF16)
    flipped = (
        jnp.dot(first, mirror, preferred_element_type=F32)
        + jnp.dot(second, mirror, preferred_element_type=F32)
        + jnp.dot(third, mirror, preferred_element_type=F32)
    )
    for h in range(2):
        low_rim = halo_recv[0, h:h + 1, :]
        high_rim = halo_recv[1, h:h + 1, :]
        sxp[h, 7:8, :] = jnp.where(g == 0, 0.0, low_rim)
        sxp[h, 40:41, :] = jnp.where(g == N_GRP - 1, -flipped[1 - h:2 - h, :], high_rim)
    west_pack, east_pack = halo_recv[2], halo_recv[3]
    lane32 = lax.broadcasted_iota(jnp.int32, (32, LANES), 1)
    west_rim = jnp.concatenate(
        [west_pack] + [pltpu.roll(west_pack, LANES - a, 1) for a in range(1, 4)], axis=0
    )
    east_rim = jnp.concatenate([pltpu.roll(east_pack, LANES - 1 - a, 1) for a in range(4)], axis=0)
    left_up, right_up = pltpu.roll(left_y, 1, 1), pltpu.roll(right_y, 1, 1)
    left_dn, right_dn = pltpu.roll(left_y, LANES - 1, 1), pltpu.roll(right_y, LANES - 1, 1)
    edge_w, edge_e = lane32 == 0, lane32 == LANES - 1
    diffs = (
        jnp.where(edge_e, right_dn, left_dn) - jnp.where(edge_w, west_rim, left_up),
        jnp.where(edge_e, east_rim, right_dn) - jnp.where(edge_w, left_up, right_up),
    )
    for h in range(2):
        column = sxp[h, 9:41, :] - sxp[h, 7:39, :]
        curl_ref[32 * h:32 * h + 32, :] = (0.5 * diffs[h] - 0.5 * column) * share[32 * h:32 * h + 32]

    for k in range(1, N_TILE):
        back[k].wait_recv()
    arrived = ret_recv[...].reshape(N_TILE * CAP * NB, LANES)
    high, low = split(arrived)
    back_ref[...] = jnp.dot(gather_back, high.astype(BF16), preferred_element_type=F32) + jnp.dot(
        gather_back, low.astype(BF16), preferred_element_type=F32
    )
    for k in FAR_FIRST:
        forward[k].wait_send()
        back[k].wait_send()
    for copy in halos:
        copy.wait_send()


def write_out(heat_ref, curl_ref, back_ref, heat_out, curl_out, atm_out):
    for h in range(2):
        heat_out[:, h * LANES:(h + 1) * LANES] = heat_ref[32 * h:32 * h + 32, :]
        curl_out[:, h * LANES:(h + 1) * LANES] = curl_ref[32 * h:32 * h + 32, :]
    for b in range(8):
        atm_out[:, b * LANES:(b + 1) * LANES] = back_ref[b * NB:(b + 1) * NB, :]


def per_device(atm_flux, send_block, send_count, recv_block, recv_weight, sea_temp, ocean_mask):
    hbm = pl.BlockSpec(memory_space=pl.ANY)
    smem = pl.BlockSpec(memory_space=pltpu.SMEM)
    vmem = pl.BlockSpec(memory_space=pltpu.VMEM)
    dma = pltpu.SemaphoreType.DMA
    heat, curl, back = pl.pallas_call(
        exchange,
        out_shape=(
            jax.ShapeDtypeStruct((64, LANES), F32),
            jax.ShapeDtypeStruct((64, LANES), F32),
            jax.ShapeDtypeStruct((32, LANES), F32),
        ),
        in_specs=[hbm, smem, smem, smem, hbm, hbm, hbm],
        out_specs=(vmem, vmem, vmem),
        scratch_shapes=[
            pltpu.VMEM((NF, 1024), F32),
            pltpu.VMEM((8, NF, LANES), F32),
            pltpu.VMEM((N_TILE, CAP, LANES, LANES), BF16),
            pltpu.VMEM((32, 256), F32),
            pltpu.VMEM((32, 256), jnp.int32),
            pltpu.VMEM((N_TILE, CAP * NF, LANES), F32),
            pltpu.VMEM((N_TILE, CAP * NF, LANES), F32),
            pltpu.VMEM((512, LANES), F32),
            pltpu.VMEM((64, 8, LANES), F32),
            pltpu.VMEM((N_TILE, CAP * NB, LANES), F32),
            pltpu.VMEM((N_TILE, CAP * NB, LANES), F32),
            pltpu.VMEM((2, 48, LANES), F32),
            pltpu.VMEM((4, 8, LANES), F32),
            pltpu.VMEM((5, 8, LANES), F32),
            dma((4,)),
            dma((N_TILE,)),
            dma((N_TILE,)),
            dma((N_TILE,)),
            dma((N_TILE,)),
            dma((5,)),
            dma((5,)),
        ],
        compiler_params=pltpu.CompilerParams(collective_id=0, has_side_effects=True),
        name="exchange",
    )(
        atm_flux,
        jnp.transpose(send_block[0], (1, 0)),
        send_count,
        jnp.transpose(recv_block[0], (1, 0)),
        recv_weight[0],
        sea_temp,
        ocean_mask,
    )
    return pl.pallas_call(
        write_out,
        out_shape=(
            jax.ShapeDtypeStruct((32, 256), F32),
            jax.ShapeDtypeStruct((32, 256), F32),
            jax.ShapeDtypeStruct((NB, 1024), F32),
        ),
        in_specs=[vmem, vmem, vmem],
        out_specs=(vmem, vmem, vmem),
        name="write_out",
    )(heat, curl, back)


def solution(mesh):
    placed = (
        P(None, ("grp", "tile")),
        P(("grp", "tile"), None, None),
        P(("grp", "tile"), None),
        P(("grp", "tile"), None, None),
        P(("grp", "tile"), None, None, None, None),
        P("grp", "tile"),
        P("grp", "tile"),
    )
    return jax.shard_map(
        per_device,
        mesh=mesh,
        in_specs=placed,
        out_specs=(P("grp", "tile"), P("grp", "tile"), P(None, ("grp", "tile"))),
        check_vma=False,
    )
```

```python
import functools

import jax
import jax.numpy as jnp
from jax import lax
from jax.experimental import pallas as pl
from jax.experimental.pallas import tpu as pltpu
from jax.sharding import PartitionSpec as P

MESH = pl.DeviceIdType.MESH
F32 = jnp.float32
BF16 = jnp.bfloat16
NZ = 8
N_TILE = 16
N_GRP = 64
CAP = 4
NF = 6
NB = 4
LANES = 128
N_PEER = 16
HALF = CAP * NF


def split(value):
    high = value.astype(BF16).astype(F32)
    return high, value - high


def exchange(
    atm_hbm, sb_hbm, sc_hbm, rb_hbm, w_hbm, temp_hbm, mask_hbm,
    heat_ref, curl_ref, back_ref,
    atm, sb_ref, sc_ref, rb_ref, tiles, w, temp, mask, send, recv, cross, pass_up, pass_over, rows, surf, ret_send, ret_recv,
    sxp, halo_send, halo_recv,
    in_sem, fs_sem, fr_sem, cs_sem, xr_sem, us_sem, ur_sem, os_sem, or_sem, bs_sem, br_sem, hs_sem, hr_sem,
    column_in, partner_in, group_in,
):
    g = lax.axis_index("grp")
    t = lax.axis_index("tile")
    half = lax.rem(t, 2)
    partner = t + 1 - 2 * half
    shift = 1 - jnp.minimum(g, 1)
    z = lax.rem(t // 2 + (NZ - 1) * shift, NZ)

    def at_level(j, column):
        return lax.rem(j + shift, NZ) * 2 + column

    def peer(k):
        return at_level(k, half) if k < NZ else at_level(k - NZ, 1 - half)

    loads = [
        pltpu.make_async_copy(atm_hbm, atm, in_sem.at[0]),
        pltpu.make_async_copy(sb_hbm, sb_ref, in_sem.at[1]),
        pltpu.make_async_copy(sc_hbm, sc_ref, in_sem.at[2]),
        pltpu.make_async_copy(rb_hbm, rb_ref, in_sem.at[3]),
        pltpu.make_async_copy(w_hbm, w, in_sem.at[4]),
        pltpu.make_async_copy(temp_hbm, temp, in_sem.at[5]),
        pltpu.make_async_copy(mask_hbm, mask, in_sem.at[6]),
    ]
    for load in loads[:4]:
        load.start()
    up, down = g < N_GRP - 1, g > 0
    last8, first8 = lax.rem(g, 8) == 7, lax.rem(g, 8) == 0
    barrier = pltpu.get_barrier_semaphore()
    for j in range(NZ - 1, 0, -1):
        @pl.when(z < j)
        def _():
            pl.semaphore_signal(barrier, 1, device_id=(g, peer(j)), device_id_type=MESH)

    @pl.when(up & jnp.logical_not(last8))
    def _():
        pl.semaphore_signal(barrier, 1, device_id=(g + 1, t), device_id_type=MESH)

    @pl.when(down & first8)
    def _():
        pl.semaphore_signal(barrier, 1, device_id=(g - 1, t), device_id_type=MESH)

    for load in loads[4:]:
        load.start()
    is_last8, not_first8 = lax.rem(g, 8) // 7, jnp.minimum(lax.rem(g, 8), 1)
    below = jnp.minimum(g, 1) * not_first8
    above = is_last8 * jnp.minimum(N_GRP - 1 - g, 1)
    earlier = z + half + below + above
    pl.when(earlier > 0)(lambda: pl.semaphore_wait(barrier, earlier))

    @pl.when(half == 0)
    def _():
        pl.semaphore_signal(barrier, 1, device_id=(g, partner), device_id_type=MESH)

    @pl.when(half == 1)
    def _():
        pl.semaphore_signal(partner_in, 1, device_id=(g, partner), device_id_type=MESH)

    for j in (3, 2, 4, 1, 5, 0, 6):
        @pl.when(z > j)
        def _():
            pl.semaphore_signal(column_in.at[z], 1, device_id=(g, peer(j)), device_id_type=MESH)

    @pl.when(up & last8)
    def _():
        pl.semaphore_signal(group_in.at[0], 1, device_id=(g + 1, t), device_id_type=MESH)

    @pl.when(down & jnp.logical_not(first8))
    def _():
        pl.semaphore_signal(group_in.at[1], 1, device_id=(g - 1, t), device_id_type=MESH)

    for load in loads[:4]:
        load.wait()
    for b in range(8):
        tiles[b] = atm[:, b * LANES:(b + 1) * LANES]
    for k in range(N_PEER):
        u = peer(k)
        count = jnp.full((NF, LANES), sc_ref[0, u], jnp.int32)
        for c in range(CAP):
            at = (k // NZ) * HALF + c * NF
            send[k % NZ, at:at + NF, :] = jnp.where(count > c, tiles[sb_ref[c, u]], 0.0)
    own, other = pl.ds(0, HALF), pl.ds(HALF, HALF)
    recv[z] = send[z, own]

    def copy_to(source, target, send_sem, recv_sem, tt):
        return pltpu.make_async_remote_copy(
            src_ref=source, dst_ref=target, send_sem=send_sem, recv_sem=recv_sem,
            device_id=(g, tt), device_id_type=MESH,
        )

    def own_copy(j):
        return copy_to(send.at[j, own], recv.at[z], fs_sem.at[j], fr_sem.at[z], peer(j))

    def own_in(j):
        return copy_to(send.at[j, own], recv.at[j], fs_sem.at[j], fr_sem.at[j], peer(j))

    def other_over(j):
        return copy_to(send.at[j, other], pass_over.at[z], cs_sem.at[j], or_sem.at[z], peer(j))

    def over_in(j):
        return copy_to(send.at[j, other], pass_over.at[j], cs_sem.at[j], or_sem.at[j], peer(j))

    def other_direct(j):
        return copy_to(send.at[j, other], cross.at[z], cs_sem.at[j], xr_sem.at[z], at_level(j, 1 - half))

    def other_up(j):
        return copy_to(send.at[j, other], pass_up.at[j], cs_sem.at[j], ur_sem.at[j], partner)

    def forward_up(j):
        return copy_to(pass_up.at[j], cross.at[z], us_sem.at[j], xr_sem.at[z], peer(j))

    def forward_over(j):
        return copy_to(pass_over.at[j], cross.at[j], os_sem.at[j], xr_sem.at[j], partner)

    for j in (3, 2, 4, 1, 5, 0, 6):
        @pl.when(z > j)
        def _():
            @pl.when(half == 0)
            def _():
                other_over(j).start()

            @pl.when(half == 1)
            def _():
                other_direct(j).start()

            own_copy(j).start()

    @pl.when(half == 0)
    def _():
        pl.semaphore_wait(partner_in, 1)

    other_direct(z).start()
    for j in range(1, NZ):
        @pl.when(z < j)
        def _():
            other_up(j).start()
    for j in range(1, NZ):
        @pl.when(z < j)
        def _():
            pl.semaphore_wait(column_in.at[j], 1)
            own_copy(j).start()
    def pass_on_up():
        for j in range(1, NZ):
            @pl.when(z < j)
            def _():
                other_up(j).wait_recv()
                forward_up(j).start()

    pl.when(z < NZ // 2)(pass_on_up)
    for j in range(1, NZ):
        @pl.when((z < j) & (half == 0))
        def _():
            over_in(j).wait_recv()
            forward_over(j).start()
    pl.when(z >= NZ // 2)(pass_on_up)

    lane = lax.broadcasted_iota(jnp.int32, (8, LANES), 1)
    dest = jnp.full((8, LANES), -1, jnp.int32)
    for k in range(N_PEER):
        for c in range(CAP):
            dest = jnp.where(lax.rem(lane, 64) == k * CAP + c, rb_ref[c, peer(k)], dest)
    row64 = lax.broadcasted_iota(jnp.int32, (64, LANES), 0)
    block_of_row = 2 * lax.rem(row64, 32) + row64 // 32
    land = jnp.where(block_of_row == jnp.concatenate([dest] * 8, axis=0), 1.0, 0.0).astype(BF16)

    for load in loads[4:]:
        load.wait()
    zeros2 = jnp.zeros((2, LANES), F32)

    def products(k):
        source = recv.at[k] if k < NZ else cross.at[k - NZ]
        for c in range(CAP):
            high, low = split(source[c * NF:(c + 1) * NF, :])
            lhs = jnp.concatenate([high, zeros2, low, zeros2], axis=0).astype(BF16)
            out = lax.dot_general(lhs, w[peer(k), c], (((1,), (1,)), ((), ())), preferred_element_type=F32)
            at = (k * CAP + c) * 8
            rows[at:at + 8, :] = out[:8] + out[8:]

    def cross_in(j):
        return copy_to(send.at[j, other], cross.at[j], cs_sem.at[j], xr_sem.at[j], partner)

    for first in (0, 4):
        for j in range(first, first + 4):
            @pl.when(z != j)
            def _():
                own_in(j).wait_recv()
        for j in range(first, first + 4):
            products(j)
    for first in (0, 4):
        for j in range(first, first + 4):
            cross_in(j).wait_recv()
        for j in range(first, first + 4):
            products(NZ + j)

    def landed(f):
        high, low = split(rows[pl.ds(f, 64, stride=8), :])
        rhs = jnp.concatenate([high, low], axis=0).astype(BF16)
        return jnp.dot(land, rhs, preferred_element_type=F32)

    surf[...] = jnp.zeros_like(surf)
    wind_u, wind_v, air_temp, air_vapor, short_down, long_down = [landed(f) for f in range(NF)]
    sea = jnp.concatenate([temp[:, :LANES], temp[:, LANES:]], axis=0)
    share = jnp.concatenate([mask[:, :LANES], mask[:, LANES:]], axis=0).astype(F32)
    speed = jnp.sqrt(wind_u * wind_u + wind_v * wind_v + 0.5)
    sensible = 0.6 * speed * (sea - air_temp)
    latent = 0.7 * speed * (jnp.exp(0.3 * sea) - air_vapor)
    base = 1.0 + 0.2 * sea
    long_up = 0.4 * ((base * base) * (base * base))
    for f, value in enumerate((sea, sensible, latent, long_up)):
        value = value * share
        for h in range(2):
            surf[pl.ds(h, 32, stride=2), f, :] = value[32 * h:32 * h + 32]

    stress_x = 0.8 * speed * wind_u * share
    stress_y = 0.8 * speed * wind_v * share
    heat_ref[...] = (0.94 * short_down + long_down - long_up - sensible - latent) * share

    left_y, right_y = stress_y[:32], stress_y[32:]
    to_east = jnp.zeros((8, LANES), F32)
    to_west = jnp.zeros((8, LANES), F32)
    for a in range(4):
        east = pltpu.roll(right_y[8 * a:8 * a + 8], a + 1, 1)
        west = left_y[8 * a:8 * a + 8]
        if a:
            west = pltpu.roll(west, a, 1)
        to_east = jnp.where(lane == a, east, to_east)
        to_west = jnp.where(lane == a, west, to_west)
    sxp[0, 8:40, :] = stress_x[:32]
    sxp[1, 8:40, :] = stress_x[32:]
    zeros6 = jnp.zeros((6, LANES), F32)
    halo_send[0] = jnp.concatenate([stress_x[31:32], stress_x[63:64], zeros6], axis=0)
    halo_send[1] = jnp.concatenate([stress_x[0:1], stress_x[32:33], zeros6], axis=0)
    halo_send[2] = to_east
    halo_send[3] = to_west
    def halo(i, source, gg, tt):
        return pltpu.make_async_remote_copy(
            src_ref=halo_send.at[source], dst_ref=halo_recv.at[i], send_sem=hs_sem.at[i], recv_sem=hr_sem.at[i],
            device_id=(gg, tt), device_id_type=MESH,
        )

    t_next, t_last = lax.rem(t + 1, N_TILE), lax.rem(t + N_TILE - 1, N_TILE)
    to_north, to_south = halo(0, 0, g + 1, t), halo(1, 1, g - 1, t)
    around = [halo(2, 2, g, t_next), halo(3, 3, g, t_last)]
    across = halo(4, 0, g, N_TILE - 1 - t)
    def send_halos():
        for copy in around:
            copy.start()
        pl.when(down & first8)(lambda: pl.semaphore_wait(group_in.at[0], 1))
        pl.when(up & jnp.logical_not(last8))(lambda: pl.semaphore_wait(group_in.at[1], 1))
        pl.when(down)(lambda: to_south.start())
        pl.when(up)(lambda: to_north.start())
        pl.when(g == N_GRP - 1)(lambda: across.start())

    def back(k):
        mine = z if k < NZ else NZ + z
        return pltpu.make_async_remote_copy(
            src_ref=ret_send.at[k], dst_ref=ret_recv.at[mine], send_sem=bs_sem.at[k], recv_sem=br_sem.at[mine],
            device_id=(g, peer(k)), device_id_type=MESH,
        )

    def back_in(k):
        return pltpu.make_async_remote_copy(
            src_ref=ret_send.at[k], dst_ref=ret_recv.at[k], send_sem=bs_sem.at[k], recv_sem=br_sem.at[k],
            device_id=(g, peer(k)), device_id_type=MESH,
        )

    def if_other(k, act):
        if k < NZ:
            pl.when(z != k)(act)
        else:
            act()

    order = [k for j in range(NZ) for k in (NZ + j, j)]
    for i, k in enumerate(order):
        for c in range(CAP):
            high, low = split(surf[rb_ref[c, peer(k)]])
            lhs = jnp.concatenate([high, low], axis=0).astype(BF16)
            out = jnp.dot(lhs, w[peer(k), c], preferred_element_type=F32)
            ret_send[k, c * NB:(c + 1) * NB, :] = out[:NB] + out[8:8 + NB]
        if i:
            if_other(order[i - 1], lambda: back(order[i - 1]).start())
        if i == 3:
            send_halos()

    if_other(order[-1], lambda: back(order[-1]).start())
    ret_recv[z] = ret_send[z]

    picks = []
    row32 = lax.broadcasted_iota(jnp.int32, (32, LANES), 0)
    lane32 = lax.broadcasted_iota(jnp.int32, (32, LANES), 1)
    for part in range(2):
        pick = jnp.full((8, LANES), -1, jnp.int32)
        for k in range(8 * part, 8 * part + 8):
            count = jnp.full((8, LANES), sc_ref[0, peer(k)], jnp.int32)
            for c in range(CAP):
                chosen = (lane // NB == (k - 8 * part) * CAP + c) & (count > c)
                pick = jnp.where(chosen, sb_ref[c, peer(k)], pick)
        pick32 = jnp.concatenate([pick] * 4, axis=0)
        hit = (row32 // NB == pick32) & (lax.rem(row32, NB) == lax.rem(lane32, NB))
        picks.append(jnp.where(hit, 1.0, 0.0).astype(BF16))
    gather_back = jnp.concatenate(picks, axis=1)

    pl.when(up)(lambda: to_south.wait_recv())
    pl.when(down)(lambda: to_north.wait_recv())
    for copy in around:
        copy.wait_recv()
    pl.when(g == N_GRP - 1)(lambda: across.wait_recv())

    fold = halo_recv[4]
    first = fold.astype(BF16)
    second = (fold - first.astype(F32)).astype(BF16)
    third = (fold - first.astype(F32) - second.astype(F32)).astype(BF16)
    ri = lax.broadcasted_iota(jnp.int32, (LANES, LANES), 0)
    ci = lax.broadcasted_iota(jnp.int32, (LANES, LANES), 1)
    mirror = jnp.where(ri + ci == LANES - 1, 1.0, 0.0).astype(BF16)
    flipped = (
        jnp.dot(first, mirror, preferred_element_type=F32)
        + jnp.dot(second, mirror, preferred_element_type=F32)
        + jnp.dot(third, mirror, preferred_element_type=F32)
    )
    for h in range(2):
        sxp[h, 7:8, :] = jnp.where(g == 0, 0.0, halo_recv[0, h:h + 1, :])
        sxp[h, 40:41, :] = jnp.where(g == N_GRP - 1, -flipped[1 - h:2 - h, :], halo_recv[1, h:h + 1, :])
    west_pack, east_pack = halo_recv[2], halo_recv[3]
    west_rim = jnp.concatenate(
        [west_pack] + [pltpu.roll(west_pack, LANES - a, 1) for a in range(1, 4)], axis=0
    )
    east_rim = jnp.concatenate([pltpu.roll(east_pack, LANES - 1 - a, 1) for a in range(4)], axis=0)
    left_up, right_up = pltpu.roll(left_y, 1, 1), pltpu.roll(right_y, 1, 1)
    left_dn, right_dn = pltpu.roll(left_y, LANES - 1, 1), pltpu.roll(right_y, LANES - 1, 1)
    edge_w, edge_e = lane32 == 0, lane32 == LANES - 1
    diffs = (
        jnp.where(edge_e, right_dn, left_dn) - jnp.where(edge_w, west_rim, left_up),
        jnp.where(edge_e, east_rim, right_dn) - jnp.where(edge_w, left_up, right_up),
    )
    for h in range(2):
        column = sxp[h, 9:41, :] - sxp[h, 7:39, :]
        curl_ref[32 * h:32 * h + 32, :] = (0.5 * diffs[h] - 0.5 * column) * share[32 * h:32 * h + 32]

    for k in range(N_PEER):
        if_other(k, lambda: back_in(k).wait_recv())
    arrived = ret_recv[...].reshape(N_TILE * CAP * NB, LANES)
    high, low = split(arrived)
    back_ref[...] = jnp.dot(gather_back, high.astype(BF16), preferred_element_type=F32) + jnp.dot(
        gather_back, low.astype(BF16), preferred_element_type=F32
    )
    for j in range(NZ):
        @pl.when(z != j)
        def _():
            own_copy(j).wait_send()

        other_direct(j).wait_send()

        @pl.when(z < j)
        def _():
            forward_up(j).wait_send()

        @pl.when((z < j) & (half == 0))
        def _():
            forward_over(j).wait_send()
    for k in range(N_PEER):
        if_other(k, lambda: back_in(k).wait_send())
    pl.when(up)(lambda: to_north.wait_send())
    pl.when(down)(lambda: to_south.wait_send())
    for copy in around:
        copy.wait_send()
    pl.when(g == N_GRP - 1)(lambda: across.wait_send())


def write_out(heat_ref, curl_ref, back_ref, heat_out, curl_out, atm_out):
    for h in range(2):
        heat_out[:, h * LANES:(h + 1) * LANES] = heat_ref[32 * h:32 * h + 32, :]
        curl_out[:, h * LANES:(h + 1) * LANES] = curl_ref[32 * h:32 * h + 32, :]
    for b in range(8):
        atm_out[:, b * LANES:(b + 1) * LANES] = back_ref[b * NB:(b + 1) * NB, :]


def per_device(atm_flux, send_block, send_count, recv_block, recv_weight, sea_temp, ocean_mask):
    hbm = pl.BlockSpec(memory_space=pl.ANY)
    vmem = pl.BlockSpec(memory_space=pltpu.VMEM)
    dma = pltpu.SemaphoreType.DMA
    heat, curl, back = pl.pallas_call(
        exchange,
        out_shape=(
            jax.ShapeDtypeStruct((64, LANES), F32),
            jax.ShapeDtypeStruct((64, LANES), F32),
            jax.ShapeDtypeStruct((32, LANES), F32),
        ),
        in_specs=[hbm] * 7,
        out_specs=(vmem, vmem, vmem),
        scratch_shapes=[
            pltpu.VMEM((NF, 1024), F32),
            pltpu.SMEM((CAP, N_TILE), jnp.int32),
            pltpu.SMEM((1, N_TILE), jnp.int32),
            pltpu.SMEM((CAP, N_TILE), jnp.int32),
            pltpu.VMEM((8, NF, LANES), F32),
            pltpu.VMEM((N_TILE, CAP, LANES, LANES), BF16),
            pltpu.VMEM((32, 256), F32),
            pltpu.VMEM((32, 256), jnp.int32),
            pltpu.VMEM((NZ, 2 * HALF, LANES), F32),
            pltpu.VMEM((NZ, HALF, LANES), F32),
            pltpu.VMEM((NZ, HALF, LANES), F32),
            pltpu.VMEM((NZ, HALF, LANES), F32),
            pltpu.VMEM((NZ, HALF, LANES), F32),
            pltpu.VMEM((512, LANES), F32),
            pltpu.VMEM((64, 8, LANES), F32),
            pltpu.VMEM((N_TILE, CAP * NB, LANES), F32),
            pltpu.VMEM((N_TILE, CAP * NB, LANES), F32),
            pltpu.VMEM((2, 48, LANES), F32),
            pltpu.VMEM((4, 8, LANES), F32),
            pltpu.VMEM((5, 8, LANES), F32),
            dma((7,)),
            dma((NZ,)),
            dma((NZ,)),
            dma((NZ,)),
            dma((NZ,)),
            dma((NZ,)),
            dma((NZ,)),
            dma((NZ,)),
            dma((NZ,)),
            dma((N_PEER,)),
            dma((N_PEER,)),
            dma((5,)),
            dma((5,)),
            pltpu.SemaphoreType.REGULAR((NZ,)),
            pltpu.SemaphoreType.REGULAR,
            pltpu.SemaphoreType.REGULAR((2,)),
        ],
        compiler_params=pltpu.CompilerParams(collective_id=0, has_side_effects=True),
        name="exchange",
    )(
        atm_flux,
        jnp.transpose(send_block[0], (1, 0)),
        send_count,
        jnp.transpose(recv_block[0], (1, 0)),
        recv_weight[0],
        sea_temp,
        ocean_mask,
    )
    return pl.pallas_call(
        write_out,
        out_shape=(
            jax.ShapeDtypeStruct((32, 256), F32),
            jax.ShapeDtypeStruct((32, 256), F32),
            jax.ShapeDtypeStruct((NB, 1024), F32),
        ),
        in_specs=[vmem, vmem, vmem],
        out_specs=(vmem, vmem, vmem),
        name="write_out",
    )(heat, curl, back)


def solution(mesh):
    placed = (
        P(None, ("grp", "tile")),
        P(("grp", "tile"), None, None),
        P(("grp", "tile"), None),
        P(("grp", "tile"), None, None),
        P(("grp", "tile"), None, None, None, None),
        P("grp", "tile"),
        P("grp", "tile"),
    )
    return jax.shard_map(
        per_device,
        mesh=mesh,
        in_specs=placed,
        out_specs=(P("grp", "tile"), P("grp", "tile"), P(None, ("grp", "tile"))),
        check_vma=False,
    )
```

```python
import functools

import jax
import jax.numpy as jnp
from jax import lax
from jax.experimental import pallas as pl
from jax.experimental.pallas import tpu as pltpu
from jax.sharding import PartitionSpec as P

MESH = pl.DeviceIdType.MESH
F32 = jnp.float32
BF16 = jnp.bfloat16
NZ = 8
N_TILE = 16
N_GRP = 64
CAP = 4
NF = 6
NB = 4
LANES = 128
N_PEER = 16
HALF = CAP * NF


def split(value):
    high = value.astype(BF16).astype(F32)
    return high, value - high


def exchange(
    atm_hbm, sb_hbm, sc_hbm, rb_hbm, w_hbm, temp_hbm, mask_hbm,
    heat_ref, curl_ref, back_ref,
    atm, sb_ref, sc_ref, rb_ref, tiles, w, temp, mask, send, recv, cross, pass_up, pass_over, rows, surf, ret_send, ret_recv,
    sxp, halo_send, halo_recv,
    in_sem, fs_sem, fr_sem, cs_sem, xr_sem, us_sem, ur_sem, os_sem, or_sem, bs_sem, br_sem, hs_sem, hr_sem,
    column_in, partner_in, group_in,
):
    g = lax.axis_index("grp")
    t = lax.axis_index("tile")
    half = lax.rem(t, 2)
    partner = t + 1 - 2 * half
    shift = 1 - jnp.minimum(g, 1)
    z = lax.rem(t // 2 + (NZ - 1) * shift, NZ)

    def at_level(j, column):
        return lax.rem(j + shift, NZ) * 2 + column

    def peer(k):
        return at_level(k, half) if k < NZ else at_level(k - NZ, 1 - half)

    loads = [
        pltpu.make_async_copy(atm_hbm, atm, in_sem.at[0]),
        pltpu.make_async_copy(sb_hbm, sb_ref, in_sem.at[1]),
        pltpu.make_async_copy(sc_hbm, sc_ref, in_sem.at[2]),
        pltpu.make_async_copy(rb_hbm, rb_ref, in_sem.at[3]),
        pltpu.make_async_copy(w_hbm, w, in_sem.at[4]),
        pltpu.make_async_copy(temp_hbm, temp, in_sem.at[5]),
        pltpu.make_async_copy(mask_hbm, mask, in_sem.at[6]),
    ]
    for load in loads[:4]:
        load.start()
    up, down = g < N_GRP - 1, g > 0
    last8, first8 = (lax.rem(g, 8) == 7) | (g == 0), (lax.rem(g, 8) == 0) | (g == 1)
    barrier = pltpu.get_barrier_semaphore()
    for j in range(NZ - 1, 0, -1):
        @pl.when(z < j)
        def _():
            pl.semaphore_signal(barrier, 1, device_id=(g, peer(j)), device_id_type=MESH)

    @pl.when(up & jnp.logical_not(last8))
    def _():
        pl.semaphore_signal(barrier, 1, device_id=(g + 1, t), device_id_type=MESH)

    @pl.when(down & first8)
    def _():
        pl.semaphore_signal(barrier, 1, device_id=(g - 1, t), device_id_type=MESH)

    for load in loads[4:]:
        load.start()
    is_last8 = lax.rem(g, 8) // 7 + shift
    not_first8 = jnp.minimum(lax.rem(g, 8), 1) * jnp.minimum(jnp.maximum(g, 1) - 1, 1)
    below = jnp.minimum(g, 1) * not_first8
    above = is_last8 * jnp.minimum(N_GRP - 1 - g, 1)
    earlier = z + half + below + above
    pl.when(earlier > 0)(lambda: pl.semaphore_wait(barrier, earlier))

    @pl.when(half == 0)
    def _():
        pl.semaphore_signal(barrier, 1, device_id=(g, partner), device_id_type=MESH)

    @pl.when(half == 1)
    def _():
        pl.semaphore_signal(partner_in, 1, device_id=(g, partner), device_id_type=MESH)

    for j in (3, 2, 4, 1, 5, 0, 6):
        @pl.when(z > j)
        def _():
            pl.semaphore_signal(column_in.at[z], 1, device_id=(g, peer(j)), device_id_type=MESH)

    @pl.when(up & last8)
    def _():
        pl.semaphore_signal(group_in.at[0], 1, device_id=(g + 1, t), device_id_type=MESH)

    @pl.when(down & jnp.logical_not(first8))
    def _():
        pl.semaphore_signal(group_in.at[1], 1, device_id=(g - 1, t), device_id_type=MESH)

    for load in loads[:4]:
        load.wait()
    for b in range(8):
        tiles[b] = atm[:, b * LANES:(b + 1) * LANES]
    for k in range(N_PEER):
        u = peer(k)
        count = jnp.full((NF, LANES), sc_ref[0, u], jnp.int32)
        for c in range(CAP):
            at = (k // NZ) * HALF + c * NF
            send[k % NZ, at:at + NF, :] = jnp.where(count > c, tiles[sb_ref[c, u]], 0.0)
    own, other = pl.ds(0, HALF), pl.ds(HALF, HALF)
    recv[z] = send[z, own]

    def copy_to(source, target, send_sem, recv_sem, tt):
        return pltpu.make_async_remote_copy(
            src_ref=source, dst_ref=target, send_sem=send_sem, recv_sem=recv_sem,
            device_id=(g, tt), device_id_type=MESH,
        )

    def own_copy(j):
        return copy_to(send.at[j, own], recv.at[z], fs_sem.at[j], fr_sem.at[z], peer(j))

    def own_in(j):
        return copy_to(send.at[j, own], recv.at[j], fs_sem.at[j], fr_sem.at[j], peer(j))

    def other_over(j):
        return copy_to(send.at[j, other], pass_over.at[z], cs_sem.at[j], or_sem.at[z], peer(j))

    def over_in(j):
        return copy_to(send.at[j, other], pass_over.at[j], cs_sem.at[j], or_sem.at[j], peer(j))

    def other_direct(j):
        return copy_to(send.at[j, other], cross.at[z], cs_sem.at[j], xr_sem.at[z], at_level(j, 1 - half))

    def other_up(j):
        return copy_to(send.at[j, other], pass_up.at[j], cs_sem.at[j], ur_sem.at[j], partner)

    def forward_up(j):
        return copy_to(pass_up.at[j], cross.at[z], us_sem.at[j], xr_sem.at[z], peer(j))

    def forward_over(j):
        return copy_to(pass_over.at[j], cross.at[j], os_sem.at[j], xr_sem.at[j], partner)

    for j in (3, 2, 4, 1, 5, 0, 6):
        @pl.when(z > j)
        def _():
            @pl.when(half == 0)
            def _():
                other_over(j).start()

            @pl.when(half == 1)
            def _():
                other_direct(j).start()

            own_copy(j).start()

    @pl.when(half == 0)
    def _():
        pl.semaphore_wait(partner_in, 1)

    other_direct(z).start()

    def push_up(j):
        pl.semaphore_wait(column_in.at[j], 1)
        own_copy(j).start()

    def pass_up_to(j):
        other_up(j).wait_recv()
        forward_up(j).start()

    def pass_over_from(j):
        @pl.when(half == 0)
        def _():
            over_in(j).wait_recv()
            forward_over(j).start()

    @pl.when(z < NZ // 2)
    def _():
        for j in range(1, NZ):
            pl.when(z < j)(lambda: other_up(j).start())
        for j in range(1, NZ):
            @pl.when(z < j)
            def _():
                push_up(j)
                pass_up_to(j)

            pl.when(z < j - 1)(lambda: pass_over_from(j - 1))
        pass_over_from(NZ - 1)

    @pl.when(z >= NZ // 2)
    def _():
        levels = range(NZ // 2 + 1, NZ)
        for j in reversed(levels):
            pl.when(z < j)(lambda: other_up(j).start())
        for j in levels:
            pl.when(z < j)(lambda: push_up(j))
        for j in levels:
            pl.when(z < j)(lambda: pass_over_from(j))
        for j in reversed(levels):
            pl.when(z < j)(lambda: pass_up_to(j))

    lane = lax.broadcasted_iota(jnp.int32, (8, LANES), 1)
    dest = jnp.full((8, LANES), -1, jnp.int32)
    for k in range(N_PEER):
        for c in range(CAP):
            dest = jnp.where(lax.rem(lane, 64) == k * CAP + c, rb_ref[c, peer(k)], dest)
    row64 = lax.broadcasted_iota(jnp.int32, (64, LANES), 0)
    block_of_row = 2 * lax.rem(row64, 32) + row64 // 32
    land = jnp.where(block_of_row == jnp.concatenate([dest] * 8, axis=0), 1.0, 0.0).astype(BF16)

    for load in loads[4:]:
        load.wait()
    zeros2 = jnp.zeros((2, LANES), F32)

    def products(k):
        source = recv.at[k] if k < NZ else cross.at[k - NZ]
        for c in range(CAP):
            high, low = split(source[c * NF:(c + 1) * NF, :])
            lhs = jnp.concatenate([high, zeros2, low, zeros2], axis=0).astype(BF16)
            out = lax.dot_general(lhs, w[peer(k), c], (((1,), (1,)), ((), ())), preferred_element_type=F32)
            at = (k * CAP + c) * 8
            rows[at:at + 8, :] = out[:8] + out[8:]

    def cross_in(j):
        return copy_to(send.at[j, other], cross.at[j], cs_sem.at[j], xr_sem.at[j], partner)

    for first in (0, 4):
        for j in range(first, first + 4):
            @pl.when(z != j)
            def _():
                own_in(j).wait_recv()
        for j in range(first, first + 4):
            products(j)
    for first in (0, 4):
        for j in range(first, first + 4):
            cross_in(j).wait_recv()
        for j in range(first, first + 4):
            products(NZ + j)

    def landed(f):
        high, low = split(rows[pl.ds(f, 64, stride=8), :])
        rhs = jnp.concatenate([high, low], axis=0).astype(BF16)
        return jnp.dot(land, rhs, preferred_element_type=F32)

    surf[...] = jnp.zeros_like(surf)
    wind_u, wind_v, air_temp, air_vapor, short_down, long_down = [landed(f) for f in range(NF)]
    sea = jnp.concatenate([temp[:, :LANES], temp[:, LANES:]], axis=0)
    share = jnp.concatenate([mask[:, :LANES], mask[:, LANES:]], axis=0).astype(F32)
    speed = jnp.sqrt(wind_u * wind_u + wind_v * wind_v + 0.5)
    sensible = 0.6 * speed * (sea - air_temp)
    latent = 0.7 * speed * (jnp.exp(0.3 * sea) - air_vapor)
    base = 1.0 + 0.2 * sea
    long_up = 0.4 * ((base * base) * (base * base))
    for f, value in enumerate((sea, sensible, latent, long_up)):
        value = value * share
        for h in range(2):
            surf[pl.ds(h, 32, stride=2), f, :] = value[32 * h:32 * h + 32]

    stress_x = 0.8 * speed * wind_u * share
    stress_y = 0.8 * speed * wind_v * share
    heat_ref[...] = (0.94 * short_down + long_down - long_up - sensible - latent) * share

    left_y, right_y = stress_y[:32], stress_y[32:]
    to_east = jnp.zeros((8, LANES), F32)
    to_west = jnp.zeros((8, LANES), F32)
    for a in range(4):
        east = pltpu.roll(right_y[8 * a:8 * a + 8], a + 1, 1)
        west = left_y[8 * a:8 * a + 8]
        if a:
            west = pltpu.roll(west, a, 1)
        to_east = jnp.where(lane == a, east, to_east)
        to_west = jnp.where(lane == a, west, to_west)
    sxp[0, 8:40, :] = stress_x[:32]
    sxp[1, 8:40, :] = stress_x[32:]
    zeros6 = jnp.zeros((6, LANES), F32)
    halo_send[0] = jnp.concatenate([stress_x[31:32], stress_x[63:64], zeros6], axis=0)
    halo_send[1] = jnp.concatenate([stress_x[0:1], stress_x[32:33], zeros6], axis=0)
    halo_send[2] = to_east
    halo_send[3] = to_west
    def halo(i, source, gg, tt):
        return pltpu.make_async_remote_copy(
            src_ref=halo_send.at[source], dst_ref=halo_recv.at[i], send_sem=hs_sem.at[i], recv_sem=hr_sem.at[i],
            device_id=(gg, tt), device_id_type=MESH,
        )

    t_next, t_last = lax.rem(t + 1, N_TILE), lax.rem(t + N_TILE - 1, N_TILE)
    to_north, to_south = halo(0, 0, g + 1, t), halo(1, 1, g - 1, t)
    around = [halo(2, 2, g, t_next), halo(3, 3, g, t_last)]
    across = halo(4, 0, g, N_TILE - 1 - t)
    def send_halos():
        for copy in around:
            copy.start()
        pl.when(down & first8)(lambda: pl.semaphore_wait(group_in.at[0], 1))
        pl.when(up & jnp.logical_not(last8))(lambda: pl.semaphore_wait(group_in.at[1], 1))
        pl.when(down)(lambda: to_south.start())
        pl.when(up)(lambda: to_north.start())
        pl.when(g == N_GRP - 1)(lambda: across.start())

    def back(k):
        mine = z if k < NZ else NZ + z
        return pltpu.make_async_remote_copy(
            src_ref=ret_send.at[k], dst_ref=ret_recv.at[mine], send_sem=bs_sem.at[k], recv_sem=br_sem.at[mine],
            device_id=(g, peer(k)), device_id_type=MESH,
        )

    def back_in(k):
        return pltpu.make_async_remote_copy(
            src_ref=ret_send.at[k], dst_ref=ret_recv.at[k], send_sem=bs_sem.at[k], recv_sem=br_sem.at[k],
            device_id=(g, peer(k)), device_id_type=MESH,
        )

    def if_other(k, act):
        if k < NZ:
            pl.when(z != k)(act)
        else:
            act()

    order = [k for j in range(NZ) for k in (NZ + j, j)]
    for i, k in enumerate(order):
        for c in range(CAP):
            high, low = split(surf[rb_ref[c, peer(k)]])
            lhs = jnp.concatenate([high, low], axis=0).astype(BF16)
            out = jnp.dot(lhs, w[peer(k), c], preferred_element_type=F32)
            ret_send[k, c * NB:(c + 1) * NB, :] = out[:NB] + out[8:8 + NB]
        if i:
            if_other(order[i - 1], lambda: back(order[i - 1]).start())
        if i == 3:
            send_halos()

    if_other(order[-1], lambda: back(order[-1]).start())
    ret_recv[z] = ret_send[z]

    picks = []
    row32 = lax.broadcasted_iota(jnp.int32, (32, LANES), 0)
    lane32 = lax.broadcasted_iota(jnp.int32, (32, LANES), 1)
    for part in range(2):
        pick = jnp.full((8, LANES), -1, jnp.int32)
        for k in range(8 * part, 8 * part + 8):
            count = jnp.full((8, LANES), sc_ref[0, peer(k)], jnp.int32)
            for c in range(CAP):
                chosen = (lane // NB == (k - 8 * part) * CAP + c) & (count > c)
                pick = jnp.where(chosen, sb_ref[c, peer(k)], pick)
        pick32 = jnp.concatenate([pick] * 4, axis=0)
        hit = (row32 // NB == pick32) & (lax.rem(row32, NB) == lax.rem(lane32, NB))
        picks.append(jnp.where(hit, 1.0, 0.0).astype(BF16))
    gather_back = jnp.concatenate(picks, axis=1)

    pl.when(up)(lambda: to_south.wait_recv())
    pl.when(down)(lambda: to_north.wait_recv())
    for copy in around:
        copy.wait_recv()
    pl.when(g == N_GRP - 1)(lambda: across.wait_recv())

    fold = halo_recv[4]
    first = fold.astype(BF16)
    second = (fold - first.astype(F32)).astype(BF16)
    third = (fold - first.astype(F32) - second.astype(F32)).astype(BF16)
    ri = lax.broadcasted_iota(jnp.int32, (LANES, LANES), 0)
    ci = lax.broadcasted_iota(jnp.int32, (LANES, LANES), 1)
    mirror = jnp.where(ri + ci == LANES - 1, 1.0, 0.0).astype(BF16)
    flipped = (
        jnp.dot(first, mirror, preferred_element_type=F32)
        + jnp.dot(second, mirror, preferred_element_type=F32)
        + jnp.dot(third, mirror, preferred_element_type=F32)
    )
    for h in range(2):
        sxp[h, 7:8, :] = jnp.where(g == 0, 0.0, halo_recv[0, h:h + 1, :])
        sxp[h, 40:41, :] = jnp.where(g == N_GRP - 1, -flipped[1 - h:2 - h, :], halo_recv[1, h:h + 1, :])
    west_pack, east_pack = halo_recv[2], halo_recv[3]
    west_rim = jnp.concatenate(
        [west_pack] + [pltpu.roll(west_pack, LANES - a, 1) for a in range(1, 4)], axis=0
    )
    east_rim = jnp.concatenate([pltpu.roll(east_pack, LANES - 1 - a, 1) for a in range(4)], axis=0)
    left_up, right_up = pltpu.roll(left_y, 1, 1), pltpu.roll(right_y, 1, 1)
    left_dn, right_dn = pltpu.roll(left_y, LANES - 1, 1), pltpu.roll(right_y, LANES - 1, 1)
    edge_w, edge_e = lane32 == 0, lane32 == LANES - 1
    diffs = (
        jnp.where(edge_e, right_dn, left_dn) - jnp.where(edge_w, west_rim, left_up),
        jnp.where(edge_e, east_rim, right_dn) - jnp.where(edge_w, left_up, right_up),
    )
    for h in range(2):
        column = sxp[h, 9:41, :] - sxp[h, 7:39, :]
        curl_ref[32 * h:32 * h + 32, :] = (0.5 * diffs[h] - 0.5 * column) * share[32 * h:32 * h + 32]

    for k in range(N_PEER):
        if_other(k, lambda: back_in(k).wait_recv())
    arrived = ret_recv[...].reshape(N_TILE * CAP * NB, LANES)
    high, low = split(arrived)
    back_ref[...] = jnp.dot(gather_back, high.astype(BF16), preferred_element_type=F32) + jnp.dot(
        gather_back, low.astype(BF16), preferred_element_type=F32
    )
    for j in range(NZ):
        @pl.when(z != j)
        def _():
            own_copy(j).wait_send()

        other_direct(j).wait_send()

        @pl.when(z < j)
        def _():
            forward_up(j).wait_send()

        @pl.when((z < j) & (half == 0))
        def _():
            forward_over(j).wait_send()
    for k in range(N_PEER):
        if_other(k, lambda: back_in(k).wait_send())
    pl.when(up)(lambda: to_north.wait_send())
    pl.when(down)(lambda: to_south.wait_send())
    for copy in around:
        copy.wait_send()
    pl.when(g == N_GRP - 1)(lambda: across.wait_send())


def write_out(heat_ref, curl_ref, back_ref, heat_out, curl_out, atm_out):
    for h in range(2):
        heat_out[:, h * LANES:(h + 1) * LANES] = heat_ref[32 * h:32 * h + 32, :]
        curl_out[:, h * LANES:(h + 1) * LANES] = curl_ref[32 * h:32 * h + 32, :]
    for b in range(8):
        atm_out[:, b * LANES:(b + 1) * LANES] = back_ref[b * NB:(b + 1) * NB, :]


def per_device(atm_flux, send_block, send_count, recv_block, recv_weight, sea_temp, ocean_mask):
    hbm = pl.BlockSpec(memory_space=pl.ANY)
    vmem = pl.BlockSpec(memory_space=pltpu.VMEM)
    dma = pltpu.SemaphoreType.DMA
    heat, curl, back = pl.pallas_call(
        exchange,
        out_shape=(
            pltpu.VMEM((64, LANES), F32),
            pltpu.VMEM((64, LANES), F32),
            pltpu.VMEM((32, LANES), F32),
        ),
        in_specs=[hbm] * 7,
        out_specs=(vmem, vmem, vmem),
        scratch_shapes=[
            pltpu.VMEM((NF, 1024), F32),
            pltpu.SMEM((CAP, N_TILE), jnp.int32),
            pltpu.SMEM((1, N_TILE), jnp.int32),
            pltpu.SMEM((CAP, N_TILE), jnp.int32),
            pltpu.VMEM((8, NF, LANES), F32),
            pltpu.VMEM((N_TILE, CAP, LANES, LANES), BF16),
            pltpu.VMEM((32, 256), F32),
            pltpu.VMEM((32, 256), jnp.int32),
            pltpu.VMEM((NZ, 2 * HALF, LANES), F32),
            pltpu.VMEM((NZ, HALF, LANES), F32),
            pltpu.VMEM((NZ, HALF, LANES), F32),
            pltpu.VMEM((NZ, HALF, LANES), F32),
            pltpu.VMEM((NZ, HALF, LANES), F32),
            pltpu.VMEM((512, LANES), F32),
            pltpu.VMEM((64, 8, LANES), F32),
            pltpu.VMEM((N_TILE, CAP * NB, LANES), F32),
            pltpu.VMEM((N_TILE, CAP * NB, LANES), F32),
            pltpu.VMEM((2, 48, LANES), F32),
            pltpu.VMEM((4, 8, LANES), F32),
            pltpu.VMEM((5, 8, LANES), F32),
            dma((7,)),
            dma((NZ,)),
            dma((NZ,)),
            dma((NZ,)),
            dma((NZ,)),
            dma((NZ,)),
            dma((NZ,)),
            dma((NZ,)),
            dma((NZ,)),
            dma((N_PEER,)),
            dma((N_PEER,)),
            dma((5,)),
            dma((5,)),
            pltpu.SemaphoreType.REGULAR((NZ,)),
            pltpu.SemaphoreType.REGULAR,
            pltpu.SemaphoreType.REGULAR((2,)),
        ],
        compiler_params=pltpu.CompilerParams(collective_id=0, has_side_effects=True),
        name="exchange",
    )(
        atm_flux,
        jnp.transpose(send_block[0], (1, 0)),
        send_count,
        jnp.transpose(recv_block[0], (1, 0)),
        recv_weight[0],
        sea_temp,
        ocean_mask,
    )
    return pl.pallas_call(
        write_out,
        out_shape=(
            jax.ShapeDtypeStruct((32, 256), F32),
            jax.ShapeDtypeStruct((32, 256), F32),
            jax.ShapeDtypeStruct((NB, 1024), F32),
        ),
        in_specs=[vmem, vmem, vmem],
        out_specs=(vmem, vmem, vmem),
        name="write_out",
    )(*[pltpu.with_memory_space_constraint(x, pltpu.VMEM) for x in (heat, curl, back)])


def solution(mesh):
    placed = (
        P(None, ("grp", "tile")),
        P(("grp", "tile"), None, None),
        P(("grp", "tile"), None),
        P(("grp", "tile"), None, None),
        P(("grp", "tile"), None, None, None, None),
        P("grp", "tile"),
        P("grp", "tile"),
    )
    return jax.shard_map(
        per_device,
        mesh=mesh,
        in_specs=placed,
        out_specs=(P("grp", "tile"), P("grp", "tile"), P(None, ("grp", "tile"))),
        check_vma=False,
    )
```

```python
import functools

import jax
import jax.numpy as jnp
from jax import lax
from jax.experimental import pallas as pl
from jax.experimental.pallas import tpu as pltpu
from jax.sharding import PartitionSpec as P

MESH = pl.DeviceIdType.MESH
F32 = jnp.float32
BF16 = jnp.bfloat16
NZ = 8
N_TILE = 16
N_GRP = 64
CAP = 4
NF = 6
NB = 4
LANES = 128
N_PEER = 16
HALF = CAP * NF


def split(value):
    high = value.astype(BF16).astype(F32)
    return high, value - high


def exchange(
    atm_hbm, sb_hbm, sc_hbm, rb_hbm, w_hbm, temp_hbm, mask_hbm,
    heat_ref, curl_ref, back_ref,
    atm, sb_ref, sc_ref, rb_ref, tiles, w, temp, mask, send, recv, cross, pass_up, pass_over, rows, surf, ret_send, ret_recv,
    sxp, halo_send, halo_recv,
    in_sem, fs_sem, fr_sem, cs_sem, xr_sem, us_sem, ur_sem, os_sem, or_sem, bs_sem, br_sem, hs_sem, hr_sem,
    column_in, partner_in, group_in,
):
    g = lax.axis_index("grp")
    t = lax.axis_index("tile")
    half = lax.rem(t, 2)
    partner = t + 1 - 2 * half
    shift = 1 - jnp.minimum(g, 1)
    z = lax.rem(t // 2 + (NZ - 1) * shift, NZ)

    def at_level(j, column):
        return lax.rem(j + shift, NZ) * 2 + column

    def peer(k):
        return at_level(k, half) if k < NZ else at_level(k - NZ, 1 - half)

    loads = [
        pltpu.make_async_copy(atm_hbm, atm, in_sem.at[0]),
        pltpu.make_async_copy(sb_hbm, sb_ref, in_sem.at[1]),
        pltpu.make_async_copy(sc_hbm, sc_ref, in_sem.at[2]),
        pltpu.make_async_copy(rb_hbm, rb_ref, in_sem.at[3]),
        pltpu.make_async_copy(w_hbm, w, in_sem.at[4]),
        pltpu.make_async_copy(temp_hbm, temp, in_sem.at[5]),
        pltpu.make_async_copy(mask_hbm, mask, in_sem.at[6]),
    ]
    for load in loads[:4]:
        load.start()
    up, down = g < N_GRP - 1, g > 0
    last8, first8 = (lax.rem(g, 8) == 7) | (g == 0), (lax.rem(g, 8) == 0) | (g == 1)
    barrier = pltpu.get_barrier_semaphore()
    for j in range(NZ - 1, 0, -1):
        @pl.when(z < j)
        def _():
            pl.semaphore_signal(barrier, 1, device_id=(g, peer(j)), device_id_type=MESH)

    @pl.when(up & jnp.logical_not(last8))
    def _():
        pl.semaphore_signal(barrier, 1, device_id=(g + 1, t), device_id_type=MESH)

    @pl.when(down & first8)
    def _():
        pl.semaphore_signal(barrier, 1, device_id=(g - 1, t), device_id_type=MESH)

    for load in loads[4:]:
        load.start()
    is_last8 = lax.rem(g, 8) // 7 + shift
    not_first8 = jnp.minimum(lax.rem(g, 8), 1) * jnp.minimum(jnp.maximum(g, 1) - 1, 1)
    below = jnp.minimum(g, 1) * not_first8
    above = is_last8 * jnp.minimum(N_GRP - 1 - g, 1)
    earlier = z + half + below + above
    pl.when(earlier > 0)(lambda: pl.semaphore_wait(barrier, earlier))

    @pl.when(half == 0)
    def _():
        pl.semaphore_signal(barrier, 1, device_id=(g, partner), device_id_type=MESH)

    @pl.when(half == 1)
    def _():
        pl.semaphore_signal(partner_in, 1, device_id=(g, partner), device_id_type=MESH)

    for j in (3, 2, 4, 1, 5, 0, 6):
        @pl.when(z > j)
        def _():
            pl.semaphore_signal(column_in.at[z], 1, device_id=(g, peer(j)), device_id_type=MESH)

    @pl.when(up & last8)
    def _():
        pl.semaphore_signal(group_in.at[0], 1, device_id=(g + 1, t), device_id_type=MESH)

    @pl.when(down & jnp.logical_not(first8))
    def _():
        pl.semaphore_signal(group_in.at[1], 1, device_id=(g - 1, t), device_id_type=MESH)

    for load in loads[:4]:
        load.wait()
    for b in range(8):
        tiles[b] = atm[:, b * LANES:(b + 1) * LANES]
    for k in range(N_PEER):
        u = peer(k)
        count = jnp.full((NF, LANES), sc_ref[0, u], jnp.int32)
        for c in range(CAP):
            at = (k // NZ) * HALF + c * NF
            send[k % NZ, at:at + NF, :] = jnp.where(count > c, tiles[sb_ref[c, u]], 0.0)
    own, other = pl.ds(0, HALF), pl.ds(HALF, HALF)
    recv[z] = send[z, own]

    def copy_to(source, target, send_sem, recv_sem, tt):
        return pltpu.make_async_remote_copy(
            src_ref=source, dst_ref=target, send_sem=send_sem, recv_sem=recv_sem,
            device_id=(g, tt), device_id_type=MESH,
        )

    def own_copy(j):
        return copy_to(send.at[j, own], recv.at[z], fs_sem.at[j], fr_sem.at[z], peer(j))

    def own_in(j):
        return copy_to(send.at[j, own], recv.at[j], fs_sem.at[j], fr_sem.at[j], peer(j))

    def other_over(j):
        return copy_to(send.at[j, other], pass_over.at[z], cs_sem.at[j], or_sem.at[z], peer(j))

    def over_in(j):
        return copy_to(send.at[j, other], pass_over.at[j], cs_sem.at[j], or_sem.at[j], peer(j))

    def other_direct(j):
        return copy_to(send.at[j, other], cross.at[z], cs_sem.at[j], xr_sem.at[z], at_level(j, 1 - half))

    def other_up(j):
        return copy_to(send.at[j, other], pass_up.at[j], cs_sem.at[j], ur_sem.at[j], partner)

    def forward_up(j):
        return copy_to(pass_up.at[j], cross.at[z], us_sem.at[j], xr_sem.at[z], peer(j))

    def forward_over(j):
        return copy_to(pass_over.at[j], cross.at[j], os_sem.at[j], xr_sem.at[j], partner)

    for j in (3, 2, 4, 1, 5, 0, 6):
        @pl.when(z > j)
        def _():
            @pl.when(half == 0)
            def _():
                other_over(j).start()

            @pl.when(half == 1)
            def _():
                other_direct(j).start()

            own_copy(j).start()

    @pl.when(half == 0)
    def _():
        pl.semaphore_wait(partner_in, 1)

    other_direct(z).start()

    def push_up(j):
        pl.semaphore_wait(column_in.at[j], 1)
        own_copy(j).start()

    def pass_up_to(j):
        other_up(j).wait_recv()
        forward_up(j).start()

    def pass_over_from(j):
        @pl.when(half == 0)
        def _():
            over_in(j).wait_recv()
            forward_over(j).start()

    @pl.when(z < NZ // 2)
    def _():
        for j in range(1, NZ):
            pl.when(z < j)(lambda: other_up(j).start())
        for j in range(1, NZ):
            @pl.when(z < j)
            def _():
                push_up(j)
                pass_up_to(j)

            pl.when(z < j - 1)(lambda: pass_over_from(j - 1))
        pass_over_from(NZ - 1)

    @pl.when(z >= NZ // 2)
    def _():
        levels = range(NZ // 2 + 1, NZ)
        for j in reversed(levels):
            pl.when(z < j)(lambda: other_up(j).start())
        for j in levels:
            pl.when(z < j)(lambda: push_up(j))
        for j in levels:
            pl.when(z < j)(lambda: pass_over_from(j))
        for j in reversed(levels):
            pl.when(z < j)(lambda: pass_up_to(j))

    lane = lax.broadcasted_iota(jnp.int32, (8, LANES), 1)
    dest = jnp.full((8, LANES), -1, jnp.int32)
    for k in range(N_PEER):
        for c in range(CAP):
            dest = jnp.where(lax.rem(lane, 64) == k * CAP + c, rb_ref[c, peer(k)], dest)
    row64 = lax.broadcasted_iota(jnp.int32, (64, LANES), 0)
    block_of_row = 2 * lax.rem(row64, 32) + row64 // 32
    land = jnp.where(block_of_row == jnp.concatenate([dest] * 8, axis=0), 1.0, 0.0).astype(BF16)

    for load in loads[4:]:
        load.wait()
    zeros2 = jnp.zeros((2, LANES), F32)

    def products(k):
        source = recv.at[k] if k < NZ else cross.at[k - NZ]
        for c in range(CAP):
            high, low = split(source[c * NF:(c + 1) * NF, :])
            lhs = jnp.concatenate([high, zeros2, low, zeros2], axis=0).astype(BF16)
            out = lax.dot_general(lhs, w[peer(k), c], (((1,), (1,)), ((), ())), preferred_element_type=F32)
            at = (k * CAP + c) * 8
            rows[at:at + 8, :] = out[:8] + out[8:]

    def cross_in(j):
        return copy_to(send.at[j, other], cross.at[j], cs_sem.at[j], xr_sem.at[j], partner)

    for first in (0, 4):
        for j in range(first, first + 4):
            @pl.when(z != j)
            def _():
                own_in(j).wait_recv()
        for j in range(first, first + 4):
            products(j)
    for first in (0, 4):
        for j in range(first, first + 4):
            cross_in(j).wait_recv()
        for j in range(first, first + 4):
            products(NZ + j)

    def landed(f):
        high, low = split(rows[pl.ds(f, 64, stride=8), :])
        rhs = jnp.concatenate([high, low], axis=0).astype(BF16)
        return jnp.dot(land, rhs, preferred_element_type=F32)

    surf[...] = jnp.zeros_like(surf)
    wind_u, wind_v, air_temp, air_vapor, short_down, long_down = [landed(f) for f in range(NF)]
    sea = jnp.concatenate([temp[:, :LANES], temp[:, LANES:]], axis=0)
    share = jnp.concatenate([mask[:, :LANES], mask[:, LANES:]], axis=0).astype(F32)
    speed = jnp.sqrt(wind_u * wind_u + wind_v * wind_v + 0.5)
    sensible = 0.6 * speed * (sea - air_temp)
    latent = 0.7 * speed * (jnp.exp(0.3 * sea) - air_vapor)
    base = 1.0 + 0.2 * sea
    long_up = 0.4 * ((base * base) * (base * base))
    for f, value in enumerate((sea, sensible, latent, long_up)):
        value = value * share
        for h in range(2):
            surf[pl.ds(h, 32, stride=2), f, :] = value[32 * h:32 * h + 32]

    stress_x = 0.8 * speed * wind_u * share
    stress_y = 0.8 * speed * wind_v * share
    heat_ref[...] = (0.94 * short_down + long_down - long_up - sensible - latent) * share

    left_y, right_y = stress_y[:32], stress_y[32:]
    to_east = jnp.zeros((8, LANES), F32)
    to_west = jnp.zeros((8, LANES), F32)
    for a in range(4):
        east = pltpu.roll(right_y[8 * a:8 * a + 8], a + 1, 1)
        west = left_y[8 * a:8 * a + 8]
        if a:
            west = pltpu.roll(west, a, 1)
        to_east = jnp.where(lane == a, east, to_east)
        to_west = jnp.where(lane == a, west, to_west)
    sxp[0, 8:40, :] = stress_x[:32]
    sxp[1, 8:40, :] = stress_x[32:]
    zeros6 = jnp.zeros((6, LANES), F32)
    halo_send[0] = jnp.concatenate([stress_x[31:32], stress_x[63:64], zeros6], axis=0)
    halo_send[1] = jnp.concatenate([stress_x[0:1], stress_x[32:33], zeros6], axis=0)
    halo_send[2] = to_east
    halo_send[3] = to_west
    def halo(i, source, gg, tt):
        return pltpu.make_async_remote_copy(
            src_ref=halo_send.at[source], dst_ref=halo_recv.at[i], send_sem=hs_sem.at[i], recv_sem=hr_sem.at[i],
            device_id=(gg, tt), device_id_type=MESH,
        )

    t_next, t_last = lax.rem(t + 1, N_TILE), lax.rem(t + N_TILE - 1, N_TILE)
    to_north, to_south = halo(0, 0, g + 1, t), halo(1, 1, g - 1, t)
    around = [halo(2, 2, g, t_next), halo(3, 3, g, t_last)]
    across = halo(4, 0, g, N_TILE - 1 - t)
    def send_halos():
        for copy in around:
            copy.start()
        pl.when(down & first8)(lambda: pl.semaphore_wait(group_in.at[0], 1))
        pl.when(up & jnp.logical_not(last8))(lambda: pl.semaphore_wait(group_in.at[1], 1))
        pl.when(down)(lambda: to_south.start())
        pl.when(up)(lambda: to_north.start())
        pl.when(g == N_GRP - 1)(lambda: across.start())

    def back(k):
        mine = z if k < NZ else NZ + z
        return pltpu.make_async_remote_copy(
            src_ref=ret_send.at[k], dst_ref=ret_recv.at[mine], send_sem=bs_sem.at[k], recv_sem=br_sem.at[mine],
            device_id=(g, peer(k)), device_id_type=MESH,
        )

    def back_in(k):
        return pltpu.make_async_remote_copy(
            src_ref=ret_send.at[k], dst_ref=ret_recv.at[k], send_sem=bs_sem.at[k], recv_sem=br_sem.at[k],
            device_id=(g, peer(k)), device_id_type=MESH,
        )

    def if_other(k, act):
        if k < NZ:
            pl.when(z != k)(act)
        else:
            act()

    order = [NZ + j for j in range(NZ)] + list(range(NZ))
    for i, k in enumerate(order):
        for c in range(CAP):
            high, low = split(surf[rb_ref[c, peer(k)]])
            lhs = jnp.concatenate([high, low], axis=0).astype(BF16)
            out = jnp.dot(lhs, w[peer(k), c], preferred_element_type=F32)
            ret_send[k, c * NB:(c + 1) * NB, :] = out[:NB] + out[8:8 + NB]
        if i:
            if_other(order[i - 1], lambda: back(order[i - 1]).start())
        if i == 3:
            send_halos()

    if_other(order[-1], lambda: back(order[-1]).start())
    ret_recv[z] = ret_send[z]

    picks = []
    row32 = lax.broadcasted_iota(jnp.int32, (32, LANES), 0)
    lane32 = lax.broadcasted_iota(jnp.int32, (32, LANES), 1)
    for part in range(2):
        pick = jnp.full((8, LANES), -1, jnp.int32)
        for k in range(8 * part, 8 * part + 8):
            count = jnp.full((8, LANES), sc_ref[0, peer(k)], jnp.int32)
            for c in range(CAP):
                chosen = (lane // NB == (k - 8 * part) * CAP + c) & (count > c)
                pick = jnp.where(chosen, sb_ref[c, peer(k)], pick)
        pick32 = jnp.concatenate([pick] * 4, axis=0)
        hit = (row32 // NB == pick32) & (lax.rem(row32, NB) == lax.rem(lane32, NB))
        picks.append(jnp.where(hit, 1.0, 0.0).astype(BF16))

    pl.when(up)(lambda: to_south.wait_recv())
    pl.when(down)(lambda: to_north.wait_recv())
    for copy in around:
        copy.wait_recv()
    pl.when(g == N_GRP - 1)(lambda: across.wait_recv())

    fold = halo_recv[4]
    first = fold.astype(BF16)
    second = (fold - first.astype(F32)).astype(BF16)
    third = (fold - first.astype(F32) - second.astype(F32)).astype(BF16)
    ri = lax.broadcasted_iota(jnp.int32, (LANES, LANES), 0)
    ci = lax.broadcasted_iota(jnp.int32, (LANES, LANES), 1)
    mirror = jnp.where(ri + ci == LANES - 1, 1.0, 0.0).astype(BF16)
    flipped = (
        jnp.dot(first, mirror, preferred_element_type=F32)
        + jnp.dot(second, mirror, preferred_element_type=F32)
        + jnp.dot(third, mirror, preferred_element_type=F32)
    )
    for h in range(2):
        sxp[h, 7:8, :] = jnp.where(g == 0, 0.0, halo_recv[0, h:h + 1, :])
        sxp[h, 40:41, :] = jnp.where(g == N_GRP - 1, -flipped[1 - h:2 - h, :], halo_recv[1, h:h + 1, :])
    west_pack, east_pack = halo_recv[2], halo_recv[3]
    west_rim = jnp.concatenate(
        [west_pack] + [pltpu.roll(west_pack, LANES - a, 1) for a in range(1, 4)], axis=0
    )
    east_rim = jnp.concatenate([pltpu.roll(east_pack, LANES - 1 - a, 1) for a in range(4)], axis=0)
    left_up, right_up = pltpu.roll(left_y, 1, 1), pltpu.roll(right_y, 1, 1)
    left_dn, right_dn = pltpu.roll(left_y, LANES - 1, 1), pltpu.roll(right_y, LANES - 1, 1)
    edge_w, edge_e = lane32 == 0, lane32 == LANES - 1
    diffs = (
        jnp.where(edge_e, right_dn, left_dn) - jnp.where(edge_w, west_rim, left_up),
        jnp.where(edge_e, east_rim, right_dn) - jnp.where(edge_w, left_up, right_up),
    )
    for h in range(2):
        column = sxp[h, 9:41, :] - sxp[h, 7:39, :]
        curl_ref[32 * h:32 * h + 32, :] = (0.5 * diffs[h] - 0.5 * column) * share[32 * h:32 * h + 32]

    for j in range(NZ):
        @pl.when(z != j)
        def _():
            own_copy(j).wait_send()

        other_direct(j).wait_send()

        @pl.when(z < j)
        def _():
            forward_up(j).wait_send()

        @pl.when((z < j) & (half == 0))
        def _():
            forward_over(j).wait_send()
    for k in range(N_PEER):
        if_other(k, lambda: back_in(k).wait_send())
    pl.when(up)(lambda: to_north.wait_send())
    pl.when(down)(lambda: to_south.wait_send())
    for copy in around:
        copy.wait_send()
    pl.when(g == N_GRP - 1)(lambda: across.wait_send())
    total = jnp.zeros((32, LANES), F32)
    for part in range(2):
        for k in range(8 * part, 8 * part + 8):
            if_other(k, lambda: back_in(k).wait_recv())
        high, low = split(ret_recv[8 * part:8 * part + 8].reshape(8 * CAP * NB, LANES))
        total += jnp.dot(picks[part], high.astype(BF16), preferred_element_type=F32)
        total += jnp.dot(picks[part], low.astype(BF16), preferred_element_type=F32)
    back_ref[...] = total


def write_out(heat_ref, curl_ref, back_ref, heat_out, curl_out, atm_out):
    for h in range(2):
        heat_out[:, h * LANES:(h + 1) * LANES] = heat_ref[32 * h:32 * h + 32, :]
        curl_out[:, h * LANES:(h + 1) * LANES] = curl_ref[32 * h:32 * h + 32, :]
    for b in range(8):
        atm_out[:, b * LANES:(b + 1) * LANES] = back_ref[b * NB:(b + 1) * NB, :]


def per_device(atm_flux, send_block, send_count, recv_block, recv_weight, sea_temp, ocean_mask):
    hbm = pl.BlockSpec(memory_space=pl.ANY)
    vmem = pl.BlockSpec(memory_space=pltpu.VMEM)
    dma = pltpu.SemaphoreType.DMA
    heat, curl, back = pl.pallas_call(
        exchange,
        out_shape=(
            pltpu.VMEM((64, LANES), F32),
            pltpu.VMEM((64, LANES), F32),
            pltpu.VMEM((32, LANES), F32),
        ),
        in_specs=[hbm] * 7,
        out_specs=(vmem, vmem, vmem),
        scratch_shapes=[
            pltpu.VMEM((NF, 1024), F32),
            pltpu.SMEM((CAP, N_TILE), jnp.int32),
            pltpu.SMEM((1, N_TILE), jnp.int32),
            pltpu.SMEM((CAP, N_TILE), jnp.int32),
            pltpu.VMEM((8, NF, LANES), F32),
            pltpu.VMEM((N_TILE, CAP, LANES, LANES), BF16),
            pltpu.VMEM((32, 256), F32),
            pltpu.VMEM((32, 256), jnp.int32),
            pltpu.VMEM((NZ, 2 * HALF, LANES), F32),
            pltpu.VMEM((NZ, HALF, LANES), F32),
            pltpu.VMEM((NZ, HALF, LANES), F32),
            pltpu.VMEM((NZ, HALF, LANES), F32),
            pltpu.VMEM((NZ, HALF, LANES), F32),
            pltpu.VMEM((512, LANES), F32),
            pltpu.VMEM((64, 8, LANES), F32),
            pltpu.VMEM((N_TILE, CAP * NB, LANES), F32),
            pltpu.VMEM((N_TILE, CAP * NB, LANES), F32),
            pltpu.VMEM((2, 48, LANES), F32),
            pltpu.VMEM((4, 8, LANES), F32),
            pltpu.VMEM((5, 8, LANES), F32),
            dma((7,)),
            dma((NZ,)),
            dma((NZ,)),
            dma((NZ,)),
            dma((NZ,)),
            dma((NZ,)),
            dma((NZ,)),
            dma((NZ,)),
            dma((NZ,)),
            dma((N_PEER,)),
            dma((N_PEER,)),
            dma((5,)),
            dma((5,)),
            pltpu.SemaphoreType.REGULAR((NZ,)),
            pltpu.SemaphoreType.REGULAR,
            pltpu.SemaphoreType.REGULAR((2,)),
        ],
        compiler_params=pltpu.CompilerParams(collective_id=0, has_side_effects=True),
        name="exchange",
    )(
        atm_flux,
        jnp.transpose(send_block[0], (1, 0)),
        send_count,
        jnp.transpose(recv_block[0], (1, 0)),
        recv_weight[0],
        sea_temp,
        ocean_mask,
    )
    return pl.pallas_call(
        write_out,
        out_shape=(
            jax.ShapeDtypeStruct((32, 256), F32),
            jax.ShapeDtypeStruct((32, 256), F32),
            jax.ShapeDtypeStruct((NB, 1024), F32),
        ),
        in_specs=[vmem, vmem, vmem],
        out_specs=(vmem, vmem, vmem),
        name="write_out",
    )(*[pltpu.with_memory_space_constraint(x, pltpu.VMEM) for x in (heat, curl, back)])


def solution(mesh):
    placed = (
        P(None, ("grp", "tile")),
        P(("grp", "tile"), None, None),
        P(("grp", "tile"), None),
        P(("grp", "tile"), None, None),
        P(("grp", "tile"), None, None, None, None),
        P("grp", "tile"),
        P("grp", "tile"),
    )
    return jax.shard_map(
        per_device,
        mesh=mesh,
        in_specs=placed,
        out_specs=(P("grp", "tile"), P("grp", "tile"), P(None, ("grp", "tile"))),
        check_vma=False,
    )
```
